32 devices in a mesh: col: 8 (over y, x, core), row: 4 (over z).
Axes of the slice: x: 2, y: 2, z: 4, core: 2. Of those that a mesh axis runs over, the one named last changes fastest.
Arguments:
- visibilities: bfloat16 [2, 8192, 4096], P(None, 'col', 'row'), may hold values from -6 to 6
- col_offsets: int32 [8], P('col'), may hold values from 0 to 15360
- row_offsets: int32 [4], replicated, may hold values from 0 to 15360
- facet_offsets: int32 [8, 2], replicated, may hold values from 0 to 16383
- facet_order: int32 [8], replicated, may hold values from 0 to 7, each once
- vis_counts: int32 [8, 4], P('col', 'row'), may hold values from 512 to 1024
Outputs:
- facet_images: float32 [8, 2, 64, 4096], P('col', None, None, 'row')
- peak: float32 [8], P('col')
The draws below stay inside these ranges and needn't reach their ends.
Inputs may be any that keep to these rules, and one draw needn't show every extreme that they name: `facet_order`: each slot names a different facet.
All inputs are finite; a program needn't handle non-finite values.
Results may differ from the reference program's by a relative error of at most 0.0078.
Values may be sent and summed in bfloat16 or wider, within the bound.
A program may use at most 128 MiB of HBM per device.

```python
import math
import jax
import jax.numpy as jnp
from jax import lax

M = 1024
FS = 4096
NG = 16384
FR = 64
NFACET = 8
N_COL = 8
N_ROW = 4


def with_ends(entries, rng, least, largest):
    extent = entries.shape
    place = [jax.random.randint(jax.random.fold_in(rng, axis), (), 0, extent[axis]) for axis in range(len(extent))]
    entries = entries.at[tuple(place)].set(least)
    longest = extent.index(max(extent))
    place[longest] = (place[longest] + 1) % extent[longest]
    return entries.at[tuple(place)].set(largest)


def steps_of(key, dims, pieces, low, high):
    gain = 1.0
    for dim, blocks in pieces:
        steps = jax.random.uniform(jax.random.fold_in(jax.random.fold_in(key, 6), dim), (blocks,), jnp.float32, low / len(pieces), high / len(pieces))
        gain = gain * jnp.repeat(jnp.exp(steps), dims[dim] // blocks).reshape((-1,) + (1,) * (len(dims) - 1 - dim))
    return gain


def noise(own_key, shape, width, reach, cuts=(), kind=jnp.bfloat16):
    result = jax.random.normal(own_key, shape, jnp.float32) * width
    if len(cuts) > 0:
        result = steps_of(own_key, shape, cuts, -0.22, 0.18) * result
    return jnp.clip(result, min=-reach, max=reach).astype(kind)


def setup_inputs(seed: int = 0) -> dict:
    arg_keys = jax.random.split(jax.random.key(seed), 7)
    return {
        "visibilities": noise(arg_keys[0], (2, N_COL * M, N_ROW * M), 1.0, 6.0, ((1, 8), (2, 4))),
        "col_offsets": with_ends(jax.random.randint(arg_keys[1], (N_COL,), 0, NG - M + 1), jax.random.fold_in(arg_keys[1], 1), 0, NG - M).astype(jnp.int32),
        "row_offsets": with_ends(jax.random.randint(arg_keys[2], (N_ROW,), 0, NG - M + 1), jax.random.fold_in(arg_keys[2], 1), 0, NG - M).astype(jnp.int32),
        "facet_offsets": with_ends(jax.random.randint(arg_keys[3], (NFACET, 2), 0, NG), jax.random.fold_in(arg_keys[3], 1), 0, NG - 1).astype(jnp.int32),
        "facet_order": jax.random.permutation(arg_keys[4], NFACET).astype(jnp.int32),
        "vis_counts": with_ends(jax.random.randint(arg_keys[5], (N_COL, N_ROW), M // 2, M + 1), jax.random.fold_in(arg_keys[5], 1), M // 2, M).astype(jnp.int32),
    }


TWO_PI = 2.0 * math.pi
BEAM_SLOPE = 0.66

def phase_table(first_ids, second_ids, factor):
    product = first_ids[:, None] * second_ids[None, :] % NG
    angles = product.astype(jnp.float32) * (TWO_PI / NG)
    return ((jnp.cos(angles) * factor).astype(jnp.bfloat16), (jnp.sin(angles) * factor).astype(jnp.bfloat16))

def complex_product(left_real, left_imag, right_real, right_imag):
    left_rows = jnp.concatenate([left_real, left_imag], axis=0)
    right_cols = jnp.concatenate([right_real, right_imag], axis=1)
    product = jnp.dot(left_rows, right_cols, preferred_element_type=jnp.float32)
    product = product.reshape(2, left_real.shape[0], 2, right_real.shape[1])
    real_part = product[0, :, 0] - product[1, :, 1]
    imag_part = product[0, :, 1] + product[1, :, 0]
    return (real_part, imag_part)

def reference(visibilities, col_offsets, row_offsets, facet_offsets, facet_order, vis_counts):
    slot_pick = (facet_order[:, None] == jnp.arange(NFACET, dtype=jnp.int32)[None, :]).astype(jnp.int32)
    slot_offsets = lax.optimization_barrier(jnp.sum(slot_pick[:, :, None] * facet_offsets[None, :, :], axis=1))
    row_ids = jnp.arange(M, dtype=jnp.int32)
    pixel_rows = jnp.arange(FR, dtype=jnp.int32) + (FS // 2 - FR // 2)
    pixel_cols = jnp.arange(FS, dtype=jnp.int32)
    grid_u = (col_offsets[:, None] + row_ids[None, :]).reshape(N_COL * M)
    first_scale = 1.0 / math.sqrt(M * N_COL)
    second_scale = 0.5 / math.sqrt(M * N_ROW)

    def add_row(running, row_index):
        column_strip = lax.dynamic_slice_in_dim(visibilities, (row_index * M).astype(jnp.int32), M, 2)
        counts_here = lax.dynamic_index_in_dim(vis_counts, row_index, 1, keepdims=False)
        live_rows = (row_ids[None, :] < counts_here[:, None]).reshape(N_COL * M)
        column_strip = jnp.where(live_rows[None, :, None], column_strip, jnp.zeros_like(column_strip))
        grid_v = lax.dynamic_index_in_dim(row_offsets, row_index, 0, keepdims=False) + row_ids

        def one_slot(slot_index):
            offsets = lax.dynamic_index_in_dim(slot_offsets, slot_index, 0, keepdims=False)
            image_rows = (offsets[0] + pixel_rows) % NG
            table_real, table_imag = phase_table(image_rows, grid_u, first_scale)
            part_real, part_imag = complex_product(table_real, table_imag, column_strip[0], column_strip[1])
            columns = jnp.stack([part_real, part_imag], axis=0).astype(jnp.bfloat16)
            image_cols = (offsets[1] + pixel_cols) % NG
            second_real, second_imag = phase_table(grid_v, image_cols, second_scale)
            out_real, out_imag = complex_product(columns[0], columns[1], second_real, second_imag)
            return jnp.stack([out_real, out_imag], axis=0)
        return (running + lax.map(one_slot, jnp.arange(NFACET, dtype=jnp.int32)), None)
    initial = jnp.zeros((NFACET, 2, FR, FS), jnp.float32)
    facet_sum, ignored = lax.scan(add_row, initial, jnp.arange(N_ROW, dtype=jnp.int32))
    beam = 1.0 - BEAM_SLOPE * (pixel_cols.astype(jnp.float32) + 0.5) / FS
    facet_images = facet_sum / beam[None, None, None, :]
    magnitude = jnp.sqrt(facet_images[:, 0] * facet_images[:, 0] + facet_images[:, 1] * facet_images[:, 1])
    peak = lax.optimization_barrier(jnp.max(magnitude, axis=(1, 2)))
    return (facet_images, peak)
```

```python
import functools
import math

import jax
import jax.numpy as jnp
from jax import lax
from jax.experimental import pallas as pl
from jax.experimental.pallas import tpu as pltpu
from jax.sharding import PartitionSpec as P

FS = 4096
NG = 16384
FR = 64
TWO_PI = 2.0 * math.pi
BEAM_SLOPE = 0.66
FINE = 32
CHUNKS = 4
MESH = pl.DeviceIdType.MESH
F32 = jnp.float32
BF16 = jnp.bfloat16


def cis(product):
    shift = (NG // 4).bit_length() - 1
    turn = product & (NG - 1)
    quadrant = (turn + NG // 8) >> shift
    rest = turn - (quadrant << shift)
    angle = rest.astype(F32) * (TWO_PI / NG)
    z = angle * angle
    sine = angle * (1.0 + z * (-1.0 / 6 + z * (1.0 / 120 + z * (-1.0 / 5040 + z * (1.0 / 362880)))))
    cosine = 1.0 + z * (-0.5 + z * (1.0 / 24 + z * (-1.0 / 720 + z * (1.0 / 40320))))
    odd = (quadrant & 1) == 1
    real = jnp.where(odd, sine, cosine)
    imag = jnp.where(odd, cosine, sine)
    real = jnp.where(((quadrant + 1) & 2) != 0, -real, real)
    imag = jnp.where((quadrant & 2) != 0, -imag, imag)
    return real, imag


def iota(shape, dim):
    return lax.broadcasted_iota(jnp.int32, shape, dim)


def kernel(
    cols, rows,
    vis_hbm, col_off, row_off, facet_off, facet_order, counts,
    image, peak,
    vis, head, fine, table, mine, pair_out, pair_in, sums, others, gathered,
    coarse2, fine2, table2, totals, peaks,
    vis_sem, pair_send, pair_recv, col_send, col_recv, row_send, row_recv, peak_send, peak_recv,
):
    m = vis.shape[1]
    width = m // CHUNKS
    chips = cols // 2
    block_cols = FS // rows
    me_col = lax.axis_index("col")
    me_row = lax.axis_index("row")
    core = lax.rem(me_col, 2)
    chip = me_col // 2
    partner = chip * 2 + 1 - core

    def peer_chip(d):
        return lax.rem(chip + d, chips) * 2 + core

    def peer_row(d):
        return lax.rem(me_row + d, rows)

    barrier = pltpu.get_barrier_semaphore()
    pl.semaphore_signal(barrier, inc=1, device_id=(partner, me_row), device_id_type=MESH)
    for d in range(1, chips):
        pl.semaphore_signal(barrier, inc=1, device_id=(peer_chip(d), me_row), device_id_type=MESH)
    for d in range(1, rows):
        pl.semaphore_signal(barrier, inc=1, device_id=(me_col, peer_row(d)), device_id_type=MESH)

    def vis_copy(k):
        part = pl.ds(k * width, width)
        return pltpu.make_async_copy(vis_hbm.at[:, :, part], vis.at[:, :, part], vis_sem.at[k])

    for k in range(CHUNKS):
        vis_copy(k).start()

    u = iota((cols, m), 1)
    slot = iota((cols, m), 0)
    start = jnp.zeros((cols, m), jnp.int32)
    for half in range(2):
        for c in range(chips):
            facet = facet_order[c * 2 + (core if half == 0 else 1 - core)]
            first = (facet_off[facet, 0] + (FS // 2 - FR // 2)) & (NG - 1)
            start = jnp.where(slot == half * chips + c, first, start)
    real, imag = cis(start * (col_off[0] + u))
    scale = jnp.where(u < counts[0, 0], 1.0 / math.sqrt(m * cols), 0.0)
    head[0] = real * scale
    head[1] = imag * scale
    real, imag = cis(iota((FR, m), 0) * (col_off[0] + iota((FR, m), 1)))
    fine[0] = real
    fine[1] = imag
    for s in range(cols):
        a, b = head[0, pl.ds(s, 1), :], head[1, pl.ds(s, 1), :]
        c, d = fine[0], fine[1]
        out = pl.ds(s * FR, FR)
        imag = a * d + b * c
        table[0, out, :] = (a * c - b * d).astype(BF16)
        table[1, out, :] = imag.astype(BF16)
        table[2, out, :] = (-imag).astype(BF16)

    pl.semaphore_wait(barrier, chips + rows - 1)

    def pair_copy(k):
        return pltpu.make_async_remote_copy(
            src_ref=pair_out.at[k], dst_ref=pair_in.at[k],
            send_sem=pair_send.at[k], recv_sem=pair_recv.at[k],
            device_id=(partner, me_row), device_id_type=MESH)

    def col_copy(k, d):
        target = lax.rem(chip + d, chips)
        return pltpu.make_async_remote_copy(
            src_ref=sums.at[k, target], dst_ref=others.at[k, d - 1],
            send_sem=col_send.at[k, d - 1], recv_sem=col_recv.at[k, d - 1],
            device_id=(target * 2 + core, me_row), device_id_type=MESH)

    def row_copy(k, origin, step):
        side = 0 if step > 0 else 1
        return pltpu.make_async_remote_copy(
            src_ref=gathered.at[k, origin], dst_ref=gathered.at[k, origin],
            send_sem=row_send.at[k, side, origin], recv_sem=row_recv.at[k, origin],
            device_id=(me_col, me_row + step), device_id_type=MESH)

    def transform(k):
        vis_copy(k).wait()
        part = pl.ds(k * width, width)
        vr, vi = vis[0, :, part], vis[1, :, part]
        dot = functools.partial(jnp.dot, preferred_element_type=F32)
        for half in (1, 0):
            own = pl.ds(half * chips * FR, chips * FR)
            tr, ti, tn = table[0, own, :], table[1, own, :], table[2, own, :]
            pr = (dot(tr, vr) + dot(tn, vi)).reshape(chips, FR, width)
            pi = (dot(tr, vi) + dot(ti, vr)).reshape(chips, FR, width)
            if half == 1:
                pair_out[k, :, pl.ds(0, FR), :] = pr.astype(BF16)
                pair_out[k, :, pl.ds(FR, FR), :] = pi.astype(BF16)
                pair_copy(k).start()
            else:
                mine[k, :, pl.ds(0, FR), :] = pr
                mine[k, :, pl.ds(FR, FR), :] = pi

    def pair_sum(k):
        pair_copy(k).wait_recv()
        sums[k] = (mine[k] + pair_in[k].astype(F32)).astype(BF16)
        for d in range(1, chips):
            col_copy(k, d).start()

    def facet_sum(k):
        total = mine[k, chip] + pair_in[k, chip].astype(F32)
        for d in range(1, chips):
            col_copy(k, d).wait_recv()
            total = total + others[k, d - 1].astype(F32)
        gathered[k, me_row] = total.astype(BF16)

        @pl.when(me_row < rows - 1)
        def _():
            row_copy(k, me_row, 1).start()

        @pl.when(me_row > 0)
        def _():
            row_copy(k, me_row, -1).start()

    def relay(k, dist):
        @pl.when(me_row - dist >= 0)
        def _():
            row_copy(k, me_row - dist, 1).wait_recv()

            @pl.when(me_row < rows - 1)
            def _():
                row_copy(k, me_row - dist, 1).start()

        @pl.when(me_row + dist < rows)
        def _():
            row_copy(k, me_row + dist, -1).wait_recv()

            @pl.when(me_row > 0)
            def _():
                row_copy(k, me_row + dist, -1).start()

    def second(k):
        left = gathered[k].reshape(rows * 2 * FR, width)
        part = pl.ds(k * width, width)
        for side in range(2):
            product = jnp.dot(left, table2[side, part, :], preferred_element_type=F32)
            if k == 0:
                totals[side] = product
            else:
                totals[side] += product

    transform(0)
    for k in range(1, CHUNKS):
        transform(k)
        pair_sum(k - 1)
    pair_sum(CHUNKS - 1)

    own_facet = facet_order[me_col]
    column0 = (facet_off[own_facet, 1] + me_row * block_cols) & (NG - 1)
    shape = (m // FINE, block_cols)
    real, imag = cis(iota(shape, 0) * FINE * (column0 + iota(shape, 1)))
    coarse2[0] = real
    coarse2[1] = imag
    shape = (FINE, block_cols)
    real, imag = cis(iota(shape, 0) * (column0 + iota(shape, 1)))
    fine2[0] = real
    fine2[1] = imag

    def row_table(h, carry):
        a, b = coarse2[0, pl.ds(h, 1), :], coarse2[1, pl.ds(h, 1), :]
        c, d = fine2[0], fine2[1]
        out = pl.ds(pl.multiple_of(h * FINE, FINE), FINE)
        table2[0, out, :] = (a * c - b * d).astype(BF16)
        table2[1, out, :] = (a * d + b * c).astype(BF16)
        return carry

    lax.fori_loop(0, m // FINE, row_table, 0)

    row_ids = iota((rows, block_cols), 0)
    offsets = jnp.zeros((rows, block_cols), jnp.int32)
    for r in range(rows):
        offsets = jnp.where(row_ids == r, row_off[r], offsets)
    lanes = iota((rows, block_cols), 1)
    beam = 1.0 - BEAM_SLOPE * ((me_row * block_cols + lanes).astype(F32) + 0.5) / FS
    gain = (0.5 / math.sqrt(m * rows)) / beam
    phase_real, phase_imag = cis(offsets * ((column0 + lanes) & (NG - 1)))
    phase_real, phase_imag = phase_real * gain, phase_imag * gain

    for step in range(CHUNKS + rows - 1):
        if step < CHUNKS:
            facet_sum(step)
        for dist in range(1, rows):
            k = step - dist
            if 0 <= k < CHUNKS:
                relay(k, dist)
                if dist == rows - 1:
                    second(k)

    out_real = jnp.zeros((FR, block_cols), F32)
    out_imag = jnp.zeros((FR, block_cols), F32)
    for r in range(rows):
        top, low = pl.ds(r * 2 * FR, FR), pl.ds(r * 2 * FR + FR, FR)
        real = totals[0, top, :] - totals[1, low, :]
        imag = totals[1, top, :] + totals[0, low, :]
        a, b = phase_real[r : r + 1], phase_imag[r : r + 1]
        out_real = out_real + (real * a - imag * b)
        out_imag = out_imag + (real * b + imag * a)
    image[0, 0] = out_real
    image[0, 1] = out_imag
    power = out_real * out_real + out_imag * out_imag
    power = jnp.max(power.reshape(FR // 8, 8, block_cols), axis=0)
    best = power[:, :128]
    for n in range(1, block_cols // 128):
        best = jnp.maximum(best, power[:, n * 128 : (n + 1) * 128])
    peaks[me_row] = jnp.sqrt(best)

    def peak_copy(d):
        return pltpu.make_async_remote_copy(
            src_ref=peaks.at[me_row], dst_ref=peaks.at[me_row],
            send_sem=peak_send.at[d - 1], recv_sem=peak_recv.at[d - 1],
            device_id=(me_col, peer_row(d)), device_id_type=MESH)

    for d in range(1, rows):
        peak_copy(d).start()

    for k in range(CHUNKS):
        pair_copy(k).wait_send()
        for d in range(1, chips):
            col_copy(k, d).wait_send()

        @pl.when(me_row < rows - 1)
        def _():
            row_copy(k, me_row, 1).wait_send()

        @pl.when(me_row > 0)
        def _():
            row_copy(k, me_row, -1).wait_send()

        for dist in range(1, rows):
            @pl.when((me_row - dist >= 0) & (me_row < rows - 1))
            def _():
                row_copy(k, me_row - dist, 1).wait_send()

            @pl.when((me_row + dist < rows) & (me_row > 0))
            def _():
                row_copy(k, me_row + dist, -1).wait_send()

    for d in range(1, rows):
        peak_copy(d).wait()
    best = peaks[0]
    for r in range(1, rows):
        best = jnp.maximum(best, peaks[r])
    peak[0] = jnp.max(best)


def local(cols, rows, visibilities, col_offsets, row_offsets, facet_offsets, facet_order, vis_counts):
    m = visibilities.shape[1]
    width = m // CHUNKS
    chips = cols // 2
    block_cols = FS // rows
    dma = pltpu.SemaphoreType.DMA
    smem = pl.BlockSpec(memory_space=pltpu.SMEM)
    return pl.pallas_call(
        functools.partial(kernel, cols, rows),
        out_shape=(
            jax.ShapeDtypeStruct((1, 2, FR, block_cols), F32),
            jax.ShapeDtypeStruct((1,), F32),
        ),
        in_specs=[pl.BlockSpec(memory_space=pl.ANY)] + [smem] * 5,
        out_specs=(pl.BlockSpec(memory_space=pltpu.VMEM), smem),
        scratch_shapes=[
            pltpu.VMEM((2, m, m), BF16),
            pltpu.VMEM((2, cols, m), F32),
            pltpu.VMEM((2, FR, m), F32),
            pltpu.VMEM((3, cols * FR, m), BF16),
            pltpu.VMEM((CHUNKS, chips, 2 * FR, width), F32),
            pltpu.VMEM((CHUNKS, chips, 2 * FR, width), BF16),
            pltpu.VMEM((CHUNKS, chips, 2 * FR, width), BF16),
            pltpu.VMEM((CHUNKS, chips, 2 * FR, width), BF16),
            pltpu.VMEM((CHUNKS, chips - 1, 2 * FR, width), BF16),
            pltpu.VMEM((CHUNKS, rows, 2 * FR, width), BF16),
            pltpu.VMEM((2, m // FINE, block_cols), F32),
            pltpu.VMEM((2, FINE, block_cols), F32),
            pltpu.VMEM((2, m, block_cols), BF16),
            pltpu.VMEM((2, rows * 2 * FR, block_cols), F32),
            pltpu.VMEM((rows, 8, 128), F32),
            dma((CHUNKS,)),
            dma((CHUNKS,)),
            dma((CHUNKS,)),
            dma((CHUNKS, chips - 1)),
            dma((CHUNKS, chips - 1)),
            dma((CHUNKS, 2, rows)),
            dma((CHUNKS, rows)),
            dma((rows - 1,)),
            dma((rows - 1,)),
        ],
        compiler_params=pltpu.CompilerParams(
            collective_id=0, has_side_effects=True, vmem_limit_bytes=60 * 1024 * 1024),
    )(visibilities, col_offsets, row_offsets, facet_offsets, facet_order, vis_counts)


def solution(mesh):
    in_specs = (P(None, "col", "row"), P("col"), P(), P(), P(), P("col", "row"))
    out_specs = (P("col", None, None, "row"), P("col"))
    body = functools.partial(local, mesh.shape["col"], mesh.shape["row"])
    return jax.shard_map(body, mesh=mesh, in_specs=in_specs, out_specs=out_specs, check_vma=False)
```

```python
import functools
import math

import jax
import jax.numpy as jnp
from jax import lax
from jax.experimental import pallas as pl
from jax.experimental.pallas import tpu as pltpu
from jax.sharding import PartitionSpec as P

FS = 4096
NG = 16384
FR = 64
TWO_PI = 2.0 * math.pi
BEAM_SLOPE = 0.66
FINE = 32
CHUNKS = 4
MESH = pl.DeviceIdType.MESH
F32 = jnp.float32
BF16 = jnp.bfloat16


def cis(product):
    shift = (NG // 4).bit_length() - 1
    turn = product & (NG - 1)
    quadrant = (turn + NG // 8) >> shift
    rest = turn - (quadrant << shift)
    angle = rest.astype(F32) * (TWO_PI / NG)
    z = angle * angle
    sine = angle * (1.0 + z * (-1.0 / 6 + z * (1.0 / 120 + z * (-1.0 / 5040 + z * (1.0 / 362880)))))
    cosine = 1.0 + z * (-0.5 + z * (1.0 / 24 + z * (-1.0 / 720 + z * (1.0 / 40320))))
    odd = (quadrant & 1) == 1
    real = jnp.where(odd, sine, cosine)
    imag = jnp.where(odd, cosine, sine)
    real = jnp.where(((quadrant + 1) & 2) != 0, -real, real)
    imag = jnp.where((quadrant & 2) != 0, -imag, imag)
    return real, imag


def iota(shape, dim):
    return lax.broadcasted_iota(jnp.int32, shape, dim)


def kernel(
    cols, rows,
    vis_hbm, *refs,
):
    small, (image, peak), scratch = refs[:5], refs[5:7], refs[7:]
    (
    col_off, row_off, facet_off, facet_order, counts, small_sem,
    vis, head, fine, table, mine, pair_out, pair_in, sums, others, gathered,
    coarse2, fine2, table2, totals, peaks,
    vis_sem, pair_send, pair_recv, col_send, col_recv, row_send, row_recv, peak_send, peak_recv,
    ) = scratch
    copies = [
        pltpu.make_async_copy(source, target, small_sem.at[n])
        for n, (source, target) in enumerate(zip(small, scratch[:5]))
    ]
    for copy in copies:
        copy.start()
    m = vis.shape[1]
    width = m // CHUNKS
    chips = cols // 2
    block_cols = FS // rows
    me_col = lax.axis_index("col")
    me_row = lax.axis_index("row")
    core = lax.rem(me_col, 2)
    chip = me_col // 2
    partner = chip * 2 + 1 - core

    def peer_chip(d):
        return lax.rem(chip + d, chips) * 2 + core

    def peer_row(d):
        return lax.rem(me_row + d, rows)

    barrier = pltpu.get_barrier_semaphore()
    pl.semaphore_signal(barrier, inc=1, device_id=(partner, me_row), device_id_type=MESH)
    for d in range(1, chips):
        pl.semaphore_signal(barrier, inc=1, device_id=(peer_chip(d), me_row), device_id_type=MESH)
    for d in range(1, rows):
        pl.semaphore_signal(barrier, inc=1, device_id=(me_col, peer_row(d)), device_id_type=MESH)

    def vis_copy(k):
        part = pl.ds(k * width, width)
        return pltpu.make_async_copy(vis_hbm.at[:, :, part], vis.at[:, :, part], vis_sem.at[k])

    for k in range(CHUNKS):
        vis_copy(k).start()

    for copy in copies:
        copy.wait()

    u = iota((cols, m), 1)
    slot = iota((cols, m), 0)
    start = jnp.zeros((cols, m), jnp.int32)
    for half in range(2):
        for c in range(chips):
            facet = facet_order[c * 2 + (core if half == 0 else 1 - core)]
            first = (facet_off[0, facet] + (FS // 2 - FR // 2)) & (NG - 1)
            start = jnp.where(slot == half * chips + c, first, start)
    real, imag = cis(start * (col_off[0] + u))
    scale = jnp.where(u < counts[0, 0], 1.0 / math.sqrt(m * cols), 0.0)
    head[0] = real * scale
    head[1] = imag * scale
    real, imag = cis(iota((FR, m), 0) * (col_off[0] + iota((FR, m), 1)))
    fine[0] = real
    fine[1] = imag
    for s in range(cols):
        a, b = head[0, pl.ds(s, 1), :], head[1, pl.ds(s, 1), :]
        c, d = fine[0], fine[1]
        half, block, at = s // chips, chips * FR, s % chips * FR
        imag = a * d + b * c
        table[half, pl.ds(at, FR), :] = (-imag).astype(BF16)
        table[half, pl.ds(block + at, FR), :] = (a * c - b * d).astype(BF16)
        table[half, pl.ds(2 * block + at, FR), :] = imag.astype(BF16)

    pl.semaphore_wait(barrier, chips + rows - 1)

    def pair_copy(k):
        return pltpu.make_async_remote_copy(
            src_ref=pair_out.at[k], dst_ref=pair_in.at[k],
            send_sem=pair_send.at[k], recv_sem=pair_recv.at[k],
            device_id=(partner, me_row), device_id_type=MESH)

    def col_copy(k, d):
        target = lax.rem(chip + d, chips)
        return pltpu.make_async_remote_copy(
            src_ref=sums.at[k, target], dst_ref=others.at[k, d - 1],
            send_sem=col_send.at[k, d - 1], recv_sem=col_recv.at[k, d - 1],
            device_id=(target * 2 + core, me_row), device_id_type=MESH)

    def row_copy(k, origin, step):
        side = 0 if step > 0 else 1
        return pltpu.make_async_remote_copy(
            src_ref=gathered.at[k, origin], dst_ref=gathered.at[k, origin],
            send_sem=row_send.at[k, side, origin], recv_sem=row_recv.at[k, origin],
            device_id=(me_col, me_row + step), device_id_type=MESH)

    def transform(k, half):
        if half == 1:
            vis_copy(k).wait()
        part = pl.ds(k * width, width)
        block = chips * FR
        dot = functools.partial(jnp.dot, preferred_element_type=F32)
        both = dot(table[half, pl.ds(block, 2 * block), :], vis[0, :, part])
        both += dot(table[half, pl.ds(0, 2 * block), :], vis[1, :, part])
        pr = both[:block].reshape(chips, FR, width)
        pi = both[block:].reshape(chips, FR, width)
        if half == 1:
            pair_out[k, :, pl.ds(0, FR), :] = pr.astype(BF16)
            pair_out[k, :, pl.ds(FR, FR), :] = pi.astype(BF16)
            pair_copy(k).start()
        else:
            mine[k, :, pl.ds(0, FR), :] = pr
            mine[k, :, pl.ds(FR, FR), :] = pi

    def pair_sum(k):
        pair_copy(k).wait_recv()
        sums[k] = (mine[k] + pair_in[k].astype(F32)).astype(BF16)
        for d in range(1, chips):
            col_copy(k, d).start()

    def facet_sum(k):
        total = mine[k, chip] + pair_in[k, chip].astype(F32)
        for d in range(1, chips):
            col_copy(k, d).wait_recv()
            total = total + others[k, d - 1].astype(F32)
        gathered[k, me_row] = total.astype(BF16)

        @pl.when(me_row < rows - 1)
        def _():
            row_copy(k, me_row, 1).start()

        @pl.when(me_row > 0)
        def _():
            row_copy(k, me_row, -1).start()

    def relay(k, dist):
        @pl.when(me_row - dist >= 0)
        def _():
            row_copy(k, me_row - dist, 1).wait_recv()

            @pl.when(me_row < rows - 1)
            def _():
                row_copy(k, me_row - dist, 1).start()

        @pl.when(me_row + dist < rows)
        def _():
            row_copy(k, me_row + dist, -1).wait_recv()

            @pl.when(me_row > 0)
            def _():
                row_copy(k, me_row + dist, -1).start()

    def second(k):
        left = gathered[k].reshape(rows * 2 * FR, width)
        part = pl.ds(k * width, width)
        for side in range(2):
            product = jnp.dot(left, table2[side, part, :], preferred_element_type=F32)
            if k == 0:
                totals[side] = product
            else:
                totals[side] += product

    transform(0, 1)
    transform(0, 0)
    for k in range(1, CHUNKS):
        transform(k, 1)
        pair_sum(k - 1)
        transform(k, 0)
    pair_sum(CHUNKS - 1)
    facet_sum(0)

    own_facet = facet_order[me_col]
    column0 = (facet_off[1, own_facet] + me_row * block_cols) & (NG - 1)
    shape = (m // FINE, block_cols)
    real, imag = cis(iota(shape, 0) * FINE * (column0 + iota(shape, 1)))
    coarse2[0] = real
    coarse2[1] = imag
    shape = (FINE, block_cols)
    real, imag = cis(iota(shape, 0) * (column0 + iota(shape, 1)))
    fine2[0] = real
    fine2[1] = imag

    def row_table(h, carry):
        a, b = coarse2[0, pl.ds(h, 1), :], coarse2[1, pl.ds(h, 1), :]
        c, d = fine2[0], fine2[1]
        out = pl.ds(pl.multiple_of(h * FINE, FINE), FINE)
        table2[0, out, :] = (a * c - b * d).astype(BF16)
        table2[1, out, :] = (a * d + b * c).astype(BF16)
        return carry

    lax.fori_loop(0, m // FINE, row_table, 0)

    row_ids = iota((rows, block_cols), 0)
    offsets = jnp.zeros((rows, block_cols), jnp.int32)
    for r in range(rows):
        offsets = jnp.where(row_ids == r, row_off[r], offsets)
    lanes = iota((rows, block_cols), 1)
    beam = 1.0 - BEAM_SLOPE * ((me_row * block_cols + lanes).astype(F32) + 0.5) / FS
    gain = (0.5 / math.sqrt(m * rows)) / beam
    phase_real, phase_imag = cis(offsets * ((column0 + lanes) & (NG - 1)))
    phase_real, phase_imag = phase_real * gain, phase_imag * gain

    for step in range(CHUNKS + rows - 1):
        if 0 < step < CHUNKS:
            facet_sum(step)
        for dist in range(1, rows):
            k = step - dist
            if 0 <= k < CHUNKS:
                relay(k, dist)
                if dist == rows - 1:
                    second(k)

    out_real = jnp.zeros((FR, block_cols), F32)
    out_imag = jnp.zeros((FR, block_cols), F32)
    for r in range(rows):
        top, low = pl.ds(r * 2 * FR, FR), pl.ds(r * 2 * FR + FR, FR)
        real = totals[0, top, :] - totals[1, low, :]
        imag = totals[1, top, :] + totals[0, low, :]
        a, b = phase_real[r : r + 1], phase_imag[r : r + 1]
        out_real = out_real + (real * a - imag * b)
        out_imag = out_imag + (real * b + imag * a)
    image[0, 0] = out_real
    image[0, 1] = out_imag
    power = out_real * out_real + out_imag * out_imag
    power = jnp.max(power.reshape(FR // 8, 8, block_cols), axis=0)
    best = power[:, :128]
    for n in range(1, block_cols // 128):
        best = jnp.maximum(best, power[:, n * 128 : (n + 1) * 128])
    peaks[me_row] = jnp.sqrt(best)

    def peak_copy(d):
        return pltpu.make_async_remote_copy(
            src_ref=peaks.at[me_row], dst_ref=peaks.at[me_row],
            send_sem=peak_send.at[d - 1], recv_sem=peak_recv.at[d - 1],
            device_id=(me_col, peer_row(d)), device_id_type=MESH)

    for d in range(1, rows):
        peak_copy(d).start()

    for k in range(CHUNKS):
        pair_copy(k).wait_send()
        for d in range(1, chips):
            col_copy(k, d).wait_send()

        @pl.when(me_row < rows - 1)
        def _():
            row_copy(k, me_row, 1).wait_send()

        @pl.when(me_row > 0)
        def _():
            row_copy(k, me_row, -1).wait_send()

        for dist in range(1, rows):
            @pl.when((me_row - dist >= 0) & (me_row < rows - 1))
            def _():
                row_copy(k, me_row - dist, 1).wait_send()

            @pl.when((me_row + dist < rows) & (me_row > 0))
            def _():
                row_copy(k, me_row + dist, -1).wait_send()

    for d in range(1, rows):
        peak_copy(d).wait()
    best = peaks[0]
    for r in range(1, rows):
        best = jnp.maximum(best, peaks[r])
    peak[0] = jnp.max(best)


def local(cols, rows, visibilities, col_offsets, row_offsets, facet_offsets, facet_order, vis_counts):
    m = visibilities.shape[1]
    width = m // CHUNKS
    chips = cols // 2
    block_cols = FS // rows
    dma = pltpu.SemaphoreType.DMA
    smem = pl.BlockSpec(memory_space=pltpu.SMEM)
    anywhere = pl.BlockSpec(memory_space=pl.ANY)
    small = (col_offsets, row_offsets, facet_offsets.T, facet_order, vis_counts)
    return pl.pallas_call(
        functools.partial(kernel, cols, rows),
        out_shape=(
            pltpu.VMEM((1, 2, FR, block_cols), F32),
            jax.ShapeDtypeStruct((1,), F32),
        ),
        in_specs=[anywhere] * 6,
        out_specs=(pl.BlockSpec(memory_space=pltpu.VMEM), smem),
        scratch_shapes=[pltpu.SMEM(x.shape, x.dtype) for x in small] + [
            dma((len(small),)),
            pltpu.VMEM((2, m, m), BF16),
            pltpu.VMEM((2, cols, m), F32),
            pltpu.VMEM((2, FR, m), F32),
            pltpu.VMEM((2, 3 * chips * FR, m), BF16),
            pltpu.VMEM((CHUNKS, chips, 2 * FR, width), F32),
            pltpu.VMEM((CHUNKS, chips, 2 * FR, width), BF16),
            pltpu.VMEM((CHUNKS, chips, 2 * FR, width), BF16),
            pltpu.VMEM((CHUNKS, chips, 2 * FR, width), BF16),
            pltpu.VMEM((CHUNKS, chips - 1, 2 * FR, width), BF16),
            pltpu.VMEM((CHUNKS, rows, 2 * FR, width), BF16),
            pltpu.VMEM((2, m // FINE, block_cols), F32),
            pltpu.VMEM((2, FINE, block_cols), F32),
            pltpu.VMEM((2, m, block_cols), BF16),
            pltpu.VMEM((2, rows * 2 * FR, block_cols), F32),
            pltpu.VMEM((rows, 8, 128), F32),
            dma((CHUNKS,)),
            dma((CHUNKS,)),
            dma((CHUNKS,)),
            dma((CHUNKS, chips - 1)),
            dma((CHUNKS, chips - 1)),
            dma((CHUNKS, 2, rows)),
            dma((CHUNKS, rows)),
            dma((rows - 1,)),
            dma((rows - 1,)),
        ],
        compiler_params=pltpu.CompilerParams(
            collective_id=0, has_side_effects=True, vmem_limit_bytes=60 * 1024 * 1024),
    )(visibilities, *small)


def solution(mesh):
    in_specs = (P(None, "col", "row"), P("col"), P(), P(), P(), P("col", "row"))
    out_specs = (P("col", None, None, "row"), P("col"))
    body = functools.partial(local, mesh.shape["col"], mesh.shape["row"])
    return jax.shard_map(body, mesh=mesh, in_specs=in_specs, out_specs=out_specs, check_vma=False)
```

```python
import functools
import math

import jax
import jax.numpy as jnp
from jax import lax
from jax.experimental import pallas as pl
from jax.experimental.pallas import tpu as pltpu
from jax.sharding import PartitionSpec as P

FS = 4096
NG = 16384
FR = 64
TWO_PI = 2.0 * math.pi
BEAM_SLOPE = 0.66
FINE = 32
CHUNKS = 8
GROUPS = 4
WIDE = CHUNKS // GROUPS
MESH = pl.DeviceIdType.MESH
F32 = jnp.float32
BF16 = jnp.bfloat16


def cis(product):
    shift = (NG // 4).bit_length() - 1
    turn = product & (NG - 1)
    quadrant = (turn + NG // 8) >> shift
    rest = turn - (quadrant << shift)
    angle = rest.astype(F32) * (TWO_PI / NG)
    z = angle * angle
    sine = angle * (1.0 + z * (-1.0 / 6 + z * (1.0 / 120 + z * (-1.0 / 5040 + z * (1.0 / 362880)))))
    cosine = 1.0 + z * (-0.5 + z * (1.0 / 24 + z * (-1.0 / 720 + z * (1.0 / 40320))))
    odd = (quadrant & 1) == 1
    real = jnp.where(odd, sine, cosine)
    imag = jnp.where(odd, cosine, sine)
    real = jnp.where(((quadrant + 1) & 2) != 0, -real, real)
    imag = jnp.where((quadrant & 2) != 0, -imag, imag)
    return real, imag


def iota(shape, dim):
    return lax.broadcasted_iota(jnp.int32, shape, dim)


def kernel(
    cols, rows,
    vis_hbm, *refs,
):
    small, (image, peak), scratch = refs[:5], refs[5:7], refs[7:]
    (
    col_off, row_off, facet_off, facet_order, counts, small_sem,
    vis, head, fine, table, mine, pair_out, pair_in, sums, others, gathered,
    coarse2, fine2, table2, totals, peaks,
    vis_sem, pair_send, pair_recv, col_send, col_recv, row_send, row_recv, peak_send, peak_recv,
    ) = scratch
    copies = [
        pltpu.make_async_copy(source, target, small_sem.at[n])
        for n, (source, target) in enumerate(zip(small, scratch[:5]))
    ]
    for copy in copies:
        copy.start()
    m = vis.shape[1]
    width = m // CHUNKS
    chips = cols // 2
    block_cols = FS // rows
    me_col = lax.axis_index("col")
    me_row = lax.axis_index("row")
    core = lax.rem(me_col, 2)
    chip = me_col // 2
    partner = chip * 2 + 1 - core

    def peer_chip(d):
        return lax.rem(chip + d, chips) * 2 + core

    def peer_row(d):
        return lax.rem(me_row + d, rows)

    barrier = pltpu.get_barrier_semaphore()
    pl.semaphore_signal(barrier, inc=1, device_id=(partner, me_row), device_id_type=MESH)
    for d in range(1, chips):
        pl.semaphore_signal(barrier, inc=1, device_id=(peer_chip(d), me_row), device_id_type=MESH)
    for d in range(1, rows):
        pl.semaphore_signal(barrier, inc=1, device_id=(me_col, peer_row(d)), device_id_type=MESH)

    def vis_copy(k):
        part = pl.ds(k * WIDE * width, WIDE * width)
        return pltpu.make_async_copy(vis_hbm.at[:, :, part], vis.at[:, :, part], vis_sem.at[k])

    for g in range(GROUPS):
        vis_copy(g).start()

    for copy in copies:
        copy.wait()

    u = iota((cols, m), 1)
    slot = iota((cols, m), 0)
    start = jnp.zeros((cols, m), jnp.int32)
    for half in range(2):
        for c in range(chips):
            facet = facet_order[c * 2 + (core if half == 0 else 1 - core)]
            first = (facet_off[0, facet] + (FS // 2 - FR // 2)) & (NG - 1)
            start = jnp.where(slot == half * chips + c, first, start)
    real, imag = cis(start * (col_off[0] + u))
    scale = jnp.where(u < counts[0, 0], 1.0 / math.sqrt(m * cols), 0.0)
    head[0] = real * scale
    head[1] = imag * scale
    real, imag = cis(iota((FR, m), 0) * (col_off[0] + iota((FR, m), 1)))
    fine[0] = real
    fine[1] = imag
    def column_table(half):
        block = chips * FR
        for at in range(chips):
            s = half * chips + at
            a, b = head[0, pl.ds(s, 1), :], head[1, pl.ds(s, 1), :]
            c, d = fine[0], fine[1]
            imag = a * d + b * c
            table[half, pl.ds(at * FR, FR), :] = (-imag).astype(BF16)
            table[half, pl.ds(block + at * FR, FR), :] = (a * c - b * d).astype(BF16)
            table[half, pl.ds(2 * block + at * FR, FR), :] = imag.astype(BF16)

    def pair_copy(k):
        return pltpu.make_async_remote_copy(
            src_ref=pair_out.at[k], dst_ref=pair_in.at[k],
            send_sem=pair_send.at[k], recv_sem=pair_recv.at[k],
            device_id=(partner, me_row), device_id_type=MESH)

    def col_copy(k, d):
        target = lax.rem(chip + d, chips)
        return pltpu.make_async_remote_copy(
            src_ref=sums.at[k, target], dst_ref=others.at[k, d - 1],
            send_sem=col_send.at[k, d - 1], recv_sem=col_recv.at[k, d - 1],
            device_id=(target * 2 + core, me_row), device_id_type=MESH)

    def row_copy(k, origin, step):
        side = 0 if step > 0 else 1
        return pltpu.make_async_remote_copy(
            src_ref=gathered.at[k, origin], dst_ref=gathered.at[k, origin],
            send_sem=row_send.at[k, side, origin], recv_sem=row_recv.at[k, origin],
            device_id=(me_col, me_row + step), device_id_type=MESH)

    def transform(first, count, half):
        part = pl.ds(first * width, count * width)
        block = chips * FR
        dot = functools.partial(jnp.dot, preferred_element_type=F32)
        both = dot(table[half, pl.ds(block, 2 * block), :], vis[0, :, part])
        both += dot(table[half, pl.ds(0, 2 * block), :], vis[1, :, part])
        for n in range(count):
            k = first + n
            piece = both[:, n * width : (n + 1) * width]
            pr = piece[:block].reshape(chips, FR, width)
            pi = piece[block:].reshape(chips, FR, width)
            if half == 1:
                pair_out[k, :, pl.ds(0, FR), :] = pr.astype(BF16)
                pair_out[k, :, pl.ds(FR, FR), :] = pi.astype(BF16)
                if k == 0:
                    pl.semaphore_wait(barrier, chips + rows - 1)
                pair_copy(k).start()
            else:
                mine[k, :, pl.ds(0, FR), :] = pr
                mine[k, :, pl.ds(FR, FR), :] = pi

    def pair_sum(k):
        pair_copy(k).wait_recv()
        sums[k] = (mine[k] + pair_in[k].astype(F32)).astype(BF16)
        for d in range(1, chips):
            col_copy(k, d).start()

    def facet_sum(k):
        total = mine[k, chip] + pair_in[k, chip].astype(F32)
        for d in range(1, chips):
            col_copy(k, d).wait_recv()
            total = total + others[k, d - 1].astype(F32)
        gathered[k, me_row] = total.astype(BF16)

        @pl.when(me_row < rows - 1)
        def _():
            row_copy(k, me_row, 1).start()

        @pl.when(me_row > 0)
        def _():
            row_copy(k, me_row, -1).start()

    def relay(k, dist):
        @pl.when(me_row - dist >= 0)
        def _():
            row_copy(k, me_row - dist, 1).wait_recv()

            @pl.when(me_row < rows - 1)
            def _():
                row_copy(k, me_row - dist, 1).start()

        @pl.when(me_row + dist < rows)
        def _():
            row_copy(k, me_row + dist, -1).wait_recv()

            @pl.when(me_row > 0)
            def _():
                row_copy(k, me_row + dist, -1).start()

    def second(g):
        left = jnp.concatenate(
            [gathered[g * WIDE + n].reshape(rows * 2 * FR, width) for n in range(WIDE)], axis=1)
        part = pl.ds(g * WIDE * width, WIDE * width)
        for side in range(2):
            product = jnp.dot(left, table2[side, part, :], preferred_element_type=F32)
            if g == 0:
                totals[side] = product
            else:
                totals[side] += product

    vis_copy(0).wait()
    column_table(1)
    transform(0, 1, 1)
    column_table(0)
    transform(0, 1, 0)
    transform(1, 1, 1)
    pair_sum(0)
    transform(1, 1, 0)
    for g in range(1, GROUPS):
        vis_copy(g).wait()
        transform(g * WIDE, WIDE, 1)
        if g == 1:
            pair_sum(1)
        else:
            for n in range(WIDE):
                pair_sum((g - 1) * WIDE + n)
        if g == GROUPS - 1:
            facet_sum(0)
        transform(g * WIDE, WIDE, 0)
    for n in range(WIDE):
        pair_sum((GROUPS - 1) * WIDE + n)
    facet_sum(1)

    own_facet = facet_order[me_col]
    column0 = (facet_off[1, own_facet] + me_row * block_cols) & (NG - 1)
    shape = (m // FINE, block_cols)
    real, imag = cis(iota(shape, 0) * FINE * (column0 + iota(shape, 1)))
    coarse2[0] = real
    coarse2[1] = imag
    shape = (FINE, block_cols)
    real, imag = cis(iota(shape, 0) * (column0 + iota(shape, 1)))
    fine2[0] = real
    fine2[1] = imag

    def row_table(h, carry):
        a, b = coarse2[0, pl.ds(h, 1), :], coarse2[1, pl.ds(h, 1), :]
        c, d = fine2[0], fine2[1]
        out = pl.ds(pl.multiple_of(h * FINE, FINE), FINE)
        table2[0, out, :] = (a * c - b * d).astype(BF16)
        table2[1, out, :] = (a * d + b * c).astype(BF16)
        return carry

    lax.fori_loop(0, m // FINE, row_table, 0)

    row_ids = iota((rows, block_cols), 0)
    offsets = jnp.zeros((rows, block_cols), jnp.int32)
    for r in range(rows):
        offsets = jnp.where(row_ids == r, row_off[r], offsets)
    lanes = iota((rows, block_cols), 1)
    beam = 1.0 - BEAM_SLOPE * ((me_row * block_cols + lanes).astype(F32) + 0.5) / FS
    gain = (0.5 / math.sqrt(m * rows)) / beam
    phase_real, phase_imag = cis(offsets * ((column0 + lanes) & (NG - 1)))
    phase_real, phase_imag = phase_real * gain, phase_imag * gain

    for step in range(CHUNKS + rows - 1):
        if 1 < step < CHUNKS:
            facet_sum(step)
        for dist in range(1, rows):
            k = step - dist
            if 0 <= k < CHUNKS:
                relay(k, dist)
                if dist == rows - 1 and k % WIDE == WIDE - 1:
                    second(k // WIDE)

    out_real = jnp.zeros((FR, block_cols), F32)
    out_imag = jnp.zeros((FR, block_cols), F32)
    for r in range(rows):
        top, low = pl.ds(r * 2 * FR, FR), pl.ds(r * 2 * FR + FR, FR)
        real = totals[0, top, :] - totals[1, low, :]
        imag = totals[1, top, :] + totals[0, low, :]
        a, b = phase_real[r : r + 1], phase_imag[r : r + 1]
        out_real = out_real + (real * a - imag * b)
        out_imag = out_imag + (real * b + imag * a)
    image[0, 0] = out_real
    image[0, 1] = out_imag
    power = out_real * out_real + out_imag * out_imag
    power = jnp.max(power.reshape(FR // 8, 8, block_cols), axis=0)
    best = power[:, :128]
    for n in range(1, block_cols // 128):
        best = jnp.maximum(best, power[:, n * 128 : (n + 1) * 128])
    peaks[me_row] = jnp.sqrt(best)

    def peak_copy(d):
        return pltpu.make_async_remote_copy(
            src_ref=peaks.at[me_row], dst_ref=peaks.at[me_row],
            send_sem=peak_send.at[d - 1], recv_sem=peak_recv.at[d - 1],
            device_id=(me_col, peer_row(d)), device_id_type=MESH)

    for d in range(1, rows):
        peak_copy(d).start()

    for k in range(CHUNKS):
        pair_copy(k).wait_send()
        for d in range(1, chips):
            col_copy(k, d).wait_send()

        @pl.when(me_row < rows - 1)
        def _():
            row_copy(k, me_row, 1).wait_send()

        @pl.when(me_row > 0)
        def _():
            row_copy(k, me_row, -1).wait_send()

        for dist in range(1, rows):
            @pl.when((me_row - dist >= 0) & (me_row < rows - 1))
            def _():
                row_copy(k, me_row - dist, 1).wait_send()

            @pl.when((me_row + dist < rows) & (me_row > 0))
            def _():
                row_copy(k, me_row + dist, -1).wait_send()

    for d in range(1, rows):
        peak_copy(d).wait()
    best = peaks[0]
    for r in range(1, rows):
        best = jnp.maximum(best, peaks[r])
    peak[0] = jnp.max(best)


def local(cols, rows, visibilities, col_offsets, row_offsets, facet_offsets, facet_order, vis_counts):
    m = visibilities.shape[1]
    width = m // CHUNKS
    chips = cols // 2
    block_cols = FS // rows
    dma = pltpu.SemaphoreType.DMA
    smem = pl.BlockSpec(memory_space=pltpu.SMEM)
    anywhere = pl.BlockSpec(memory_space=pl.ANY)
    small = (col_offsets, row_offsets, facet_offsets.T, facet_order, vis_counts)
    return pl.pallas_call(
        functools.partial(kernel, cols, rows),
        out_shape=(
            pltpu.VMEM((1, 2, FR, block_cols), F32),
            jax.ShapeDtypeStruct((1,), F32),
        ),
        in_specs=[anywhere] * 6,
        out_specs=(pl.BlockSpec(memory_space=pltpu.VMEM), smem),
        scratch_shapes=[pltpu.SMEM(x.shape, x.dtype) for x in small] + [
            dma((len(small),)),
            pltpu.VMEM((2, m, m), BF16),
            pltpu.VMEM((2, cols, m), F32),
            pltpu.VMEM((2, FR, m), F32),
            pltpu.VMEM((2, 3 * chips * FR, m), BF16),
            pltpu.VMEM((CHUNKS, chips, 2 * FR, width), F32),
            pltpu.VMEM((CHUNKS, chips, 2 * FR, width), BF16),
            pltpu.VMEM((CHUNKS, chips, 2 * FR, width), BF16),
            pltpu.VMEM((CHUNKS, chips, 2 * FR, width), BF16),
            pltpu.VMEM((CHUNKS, chips - 1, 2 * FR, width), BF16),
            pltpu.VMEM((CHUNKS, rows, 2 * FR, width), BF16),
            pltpu.VMEM((2, m // FINE, block_cols), F32),
            pltpu.VMEM((2, FINE, block_cols), F32),
            pltpu.VMEM((2, m, block_cols), BF16),
            pltpu.VMEM((2, rows * 2 * FR, block_cols), F32),
            pltpu.VMEM((rows, 8, 128), F32),
            dma((GROUPS,)),
            dma((CHUNKS,)),
            dma((CHUNKS,)),
            dma((CHUNKS, chips - 1)),
            dma((CHUNKS, chips - 1)),
            dma((CHUNKS, 2, rows)),
            dma((CHUNKS, rows)),
            dma((rows - 1,)),
            dma((rows - 1,)),
        ],
        compiler_params=pltpu.CompilerParams(
            collective_id=0, has_side_effects=True, vmem_limit_bytes=60 * 1024 * 1024),
    )(visibilities, *small)


def solution(mesh):
    in_specs = (P(None, "col", "row"), P("col"), P(), P(), P(), P("col", "row"))
    out_specs = (P("col", None, None, "row"), P("col"))
    body = functools.partial(local, mesh.shape["col"], mesh.shape["row"])
    return jax.shard_map(body, mesh=mesh, in_specs=in_specs, out_specs=out_specs, check_vma=False)
```

```python
import functools
import math

import jax
import jax.numpy as jnp
from jax import lax
from jax.experimental import pallas as pl
from jax.experimental.pallas import tpu as pltpu
from jax.sharding import PartitionSpec as P

FS = 4096
NG = 16384
FR = 64
TWO_PI = 2.0 * math.pi
BEAM_SLOPE = 0.66
FINE = 32
CHUNKS = 4
MESH = pl.DeviceIdType.MESH
F32 = jnp.float32
BF16 = jnp.bfloat16


def cis(product):
    shift = (NG // 4).bit_length() - 1
    turn = product & (NG - 1)
    quadrant = (turn + NG // 8) >> shift
    rest = turn - (quadrant << shift)
    angle = rest.astype(F32) * (TWO_PI / NG)
    z = angle * angle
    sine = angle * (1.0 + z * (-1.0 / 6 + z * (1.0 / 120 + z * (-1.0 / 5040 + z * (1.0 / 362880)))))
    cosine = 1.0 + z * (-0.5 + z * (1.0 / 24 + z * (-1.0 / 720 + z * (1.0 / 40320))))
    odd = (quadrant & 1) == 1
    real = jnp.where(odd, sine, cosine)
    imag = jnp.where(odd, cosine, sine)
    real = jnp.where(((quadrant + 1) & 2) != 0, -real, real)
    imag = jnp.where((quadrant & 2) != 0, -imag, imag)
    return real, imag


def iota(shape, dim):
    return lax.broadcasted_iota(jnp.int32, shape, dim)


def kernel(
    cols, rows,
    vis_hbm, *refs,
):
    small, (image, peak), scratch = refs[:5], refs[5:7], refs[7:]
    (
    col_off, row_off, facet_off, facet_order, counts, small_sem,
    vis, head, fine, table, mine, pair_out, pair_in, sums, others, gathered,
    coarse2, fine2, table2, totals, peaks,
    vis_sem, pair_send, pair_recv, col_send, col_recv, row_send, row_recv, peak_send, peak_recv,
    ) = scratch
    copies = [
        pltpu.make_async_copy(source, target, small_sem.at[n])
        for n, (source, target) in enumerate(zip(small, scratch[:5]))
    ]
    for copy in copies:
        copy.start()
    m = vis.shape[1]
    width = m // CHUNKS
    chips = cols // 2
    block_cols = FS // rows
    me_col = lax.axis_index("col")
    me_row = lax.axis_index("row")
    core = lax.rem(me_col, 2)
    chip = me_col // 2
    partner = chip * 2 + 1 - core

    def peer_chip(d):
        return lax.rem(chip + d, chips) * 2 + core

    def peer_row(d):
        return lax.rem(me_row + d, rows)

    barrier = pltpu.get_barrier_semaphore()
    pl.semaphore_signal(barrier, inc=1, device_id=(partner, me_row), device_id_type=MESH)
    for d in range(1, chips):
        pl.semaphore_signal(barrier, inc=1, device_id=(peer_chip(d), me_row), device_id_type=MESH)
    for d in range(1, rows):
        pl.semaphore_signal(barrier, inc=1, device_id=(me_col, peer_row(d)), device_id_type=MESH)

    def vis_copy(k):
        part = pl.ds(k * width, width)
        return pltpu.make_async_copy(vis_hbm.at[:, :, part], vis.at[:, :, part], vis_sem.at[k])

    for k in range(CHUNKS):
        vis_copy(k).start()

    for copy in copies:
        copy.wait()

    u = iota((cols, m), 1)
    slot = iota((cols, m), 0)
    start = jnp.zeros((cols, m), jnp.int32)
    for half in range(2):
        for c in range(chips):
            facet = facet_order[c * 2 + (core if half == 0 else 1 - core)]
            first = (facet_off[0, facet] + (FS // 2 - FR // 2)) & (NG - 1)
            start = jnp.where(slot == half * chips + c, first, start)
    real, imag = cis(start * (col_off[0] + u))
    scale = jnp.where(u < counts[0, 0], 1.0 / math.sqrt(m * cols), 0.0)
    head[0] = real * scale
    head[1] = imag * scale
    real, imag = cis(iota((FR, m), 0) * (col_off[0] + iota((FR, m), 1)))
    fine[0] = real
    fine[1] = imag
    def column_table(half):
        block = chips * FR
        for at in range(chips):
            s = half * chips + at
            a, b = head[0, pl.ds(s, 1), :], head[1, pl.ds(s, 1), :]
            c, d = fine[0], fine[1]
            imag = a * d + b * c
            table[half, pl.ds(at * FR, FR), :] = (-imag).astype(BF16)
            table[half, pl.ds(block + at * FR, FR), :] = (a * c - b * d).astype(BF16)
            table[half, pl.ds(2 * block + at * FR, FR), :] = imag.astype(BF16)

    def pair_copy(k):
        return pltpu.make_async_remote_copy(
            src_ref=pair_out.at[k], dst_ref=pair_in.at[k],
            send_sem=pair_send.at[k], recv_sem=pair_recv.at[k],
            device_id=(partner, me_row), device_id_type=MESH)

    def col_copy(k, d):
        target = lax.rem(chip + d, chips)
        return pltpu.make_async_remote_copy(
            src_ref=sums.at[k, target], dst_ref=others.at[k, d - 1],
            send_sem=col_send.at[k, d - 1], recv_sem=col_recv.at[k, d - 1],
            device_id=(target * 2 + core, me_row), device_id_type=MESH)

    def row_copy(k, origin, step):
        side = 0 if step > 0 else 1
        return pltpu.make_async_remote_copy(
            src_ref=gathered.at[k, origin], dst_ref=gathered.at[k, origin],
            send_sem=row_send.at[k, side, origin], recv_sem=row_recv.at[k, origin],
            device_id=(me_col, me_row + step), device_id_type=MESH)

    def transform(k, half):
        if half == 1:
            vis_copy(k).wait()
        part = pl.ds(k * width, width)
        block = chips * FR
        dot = functools.partial(jnp.dot, preferred_element_type=F32)
        both = dot(table[half, pl.ds(block, 2 * block), :], vis[0, :, part])
        both += dot(table[half, pl.ds(0, 2 * block), :], vis[1, :, part])
        pr = both[:block].reshape(chips, FR, width)
        pi = both[block:].reshape(chips, FR, width)
        if half == 1:
            pair_out[k, :, pl.ds(0, FR), :] = pr.astype(BF16)
            pair_out[k, :, pl.ds(FR, FR), :] = pi.astype(BF16)
            if k == 0:
                pl.semaphore_wait(barrier, chips + rows - 1)
            pair_copy(k).start()
        else:
            mine[k, :, pl.ds(0, FR), :] = pr
            mine[k, :, pl.ds(FR, FR), :] = pi

    def pair_sum(k):
        pair_copy(k).wait_recv()
        sums[k] = (mine[k] + pair_in[k].astype(F32)).astype(BF16)
        for d in range(1, chips):
            col_copy(k, d).start()

    def facet_sum(k):
        total = mine[k, chip] + pair_in[k, chip].astype(F32)
        for d in range(1, chips):
            col_copy(k, d).wait_recv()
            total = total + others[k, d - 1].astype(F32)
        gathered[k, me_row] = total.astype(BF16)

        @pl.when(me_row < rows - 1)
        def _():
            row_copy(k, me_row, 1).start()

        @pl.when(me_row > 0)
        def _():
            row_copy(k, me_row, -1).start()

    def relay(k, dist):
        @pl.when(me_row - dist >= 0)
        def _():
            row_copy(k, me_row - dist, 1).wait_recv()

            @pl.when(me_row < rows - 1)
            def _():
                row_copy(k, me_row - dist, 1).start()

        @pl.when(me_row + dist < rows)
        def _():
            row_copy(k, me_row + dist, -1).wait_recv()

            @pl.when(me_row > 0)
            def _():
                row_copy(k, me_row + dist, -1).start()

    def second(k):
        left = gathered[k].reshape(rows * 2 * FR, width)
        part = pl.ds(k * width, width)
        for side in range(2):
            product = jnp.dot(left, table2[side, part, :], preferred_element_type=F32)
            if k == 0:
                totals[side] = product
            else:
                totals[side] += product

    column_table(1)
    transform(0, 1)
    column_table(0)
    transform(0, 0)
    for k in range(1, CHUNKS):
        transform(k, 1)
        pair_sum(k - 1)
        transform(k, 0)
    pair_sum(CHUNKS - 1)
    facet_sum(0)

    own_facet = facet_order[me_col]
    column0 = (facet_off[1, own_facet] + me_row * block_cols) & (NG - 1)
    shape = (m // FINE, block_cols)
    real, imag = cis(iota(shape, 0) * FINE * (column0 + iota(shape, 1)))
    coarse2[0] = real
    coarse2[1] = imag
    shape = (FINE, block_cols)
    real, imag = cis(iota(shape, 0) * (column0 + iota(shape, 1)))
    fine2[0] = real
    fine2[1] = imag

    def row_table(h, carry):
        a, b = coarse2[0, pl.ds(h, 1), :], coarse2[1, pl.ds(h, 1), :]
        c, d = fine2[0], fine2[1]
        out = pl.ds(pl.multiple_of(h * FINE, FINE), FINE)
        table2[0, out, :] = (a * c - b * d).astype(BF16)
        table2[1, out, :] = (a * d + b * c).astype(BF16)
        return carry

    lax.fori_loop(0, m // FINE, row_table, 0)

    row_ids = iota((rows, block_cols), 0)
    offsets = jnp.zeros((rows, block_cols), jnp.int32)
    for r in range(rows):
        offsets = jnp.where(row_ids == r, row_off[r], offsets)
    lanes = iota((rows, block_cols), 1)
    beam = 1.0 - BEAM_SLOPE * ((me_row * block_cols + lanes).astype(F32) + 0.5) / FS
    gain = (0.5 / math.sqrt(m * rows)) / beam
    phase_real, phase_imag = cis(offsets * ((column0 + lanes) & (NG - 1)))
    phase_real, phase_imag = phase_real * gain, phase_imag * gain

    for step in range(CHUNKS + rows - 1):
        if 0 < step < CHUNKS:
            facet_sum(step)
        for dist in range(1, rows):
            k = step - dist
            if 0 <= k < CHUNKS:
                relay(k, dist)
                if dist == rows - 1:
                    second(k)

    out_real = jnp.zeros((FR, block_cols), F32)
    out_imag = jnp.zeros((FR, block_cols), F32)
    for r in range(rows):
        top, low = pl.ds(r * 2 * FR, FR), pl.ds(r * 2 * FR + FR, FR)
        real = totals[0, top, :] - totals[1, low, :]
        imag = totals[1, top, :] + totals[0, low, :]
        a, b = phase_real[r : r + 1], phase_imag[r : r + 1]
        out_real = out_real + (real * a - imag * b)
        out_imag = out_imag + (real * b + imag * a)
    image[0, 0] = out_real
    image[0, 1] = out_imag
    power = out_real * out_real + out_imag * out_imag
    power = jnp.max(power.reshape(FR // 8, 8, block_cols), axis=0)
    best = power[:, :128]
    for n in range(1, block_cols // 128):
        best = jnp.maximum(best, power[:, n * 128 : (n + 1) * 128])
    peaks[me_row] = jnp.sqrt(best)

    def peak_copy(d):
        return pltpu.make_async_remote_copy(
            src_ref=peaks.at[me_row], dst_ref=peaks.at[me_row],
            send_sem=peak_send.at[d - 1], recv_sem=peak_recv.at[d - 1],
            device_id=(me_col, peer_row(d)), device_id_type=MESH)

    for d in range(1, rows):
        peak_copy(d).start()

    for k in range(CHUNKS):
        pair_copy(k).wait_send()
        for d in range(1, chips):
            col_copy(k, d).wait_send()

        @pl.when(me_row < rows - 1)
        def _():
            row_copy(k, me_row, 1).wait_send()

        @pl.when(me_row > 0)
        def _():
            row_copy(k, me_row, -1).wait_send()

        for dist in range(1, rows):
            @pl.when((me_row - dist >= 0) & (me_row < rows - 1))
            def _():
                row_copy(k, me_row - dist, 1).wait_send()

            @pl.when((me_row + dist < rows) & (me_row > 0))
            def _():
                row_copy(k, me_row + dist, -1).wait_send()

    for d in range(1, rows):
        peak_copy(d).wait()
    best = peaks[0]
    for r in range(1, rows):
        best = jnp.maximum(best, peaks[r])
    peak[0] = jnp.max(best)


def local(cols, rows, visibilities, col_offsets, row_offsets, facet_offsets, facet_order, vis_counts):
    m = visibilities.shape[1]
    width = m // CHUNKS
    chips = cols // 2
    block_cols = FS // rows
    dma = pltpu.SemaphoreType.DMA
    smem = pl.BlockSpec(memory_space=pltpu.SMEM)
    anywhere = pl.BlockSpec(memory_space=pl.ANY)
    small = (col_offsets, row_offsets, facet_offsets.T, facet_order, vis_counts)
    return pl.pallas_call(
        functools.partial(kernel, cols, rows),
        out_shape=(
            pltpu.VMEM((1, 2, FR, block_cols), F32),
            jax.ShapeDtypeStruct((1,), F32),
        ),
        in_specs=[anywhere] * 6,
        out_specs=(pl.BlockSpec(memory_space=pltpu.VMEM), smem),
        scratch_shapes=[pltpu.SMEM(x.shape, x.dtype) for x in small] + [
            dma((len(small),)),
            pltpu.VMEM((2, m, m), BF16),
            pltpu.VMEM((2, cols, m), F32),
            pltpu.VMEM((2, FR, m), F32),
            pltpu.VMEM((2, 3 * chips * FR, m), BF16),
            pltpu.VMEM((CHUNKS, chips, 2 * FR, width), F32),
            pltpu.VMEM((CHUNKS, chips, 2 * FR, width), BF16),
            pltpu.VMEM((CHUNKS, chips, 2 * FR, width), BF16),
            pltpu.VMEM((CHUNKS, chips, 2 * FR, width), BF16),
            pltpu.VMEM((CHUNKS, chips - 1, 2 * FR, width), BF16),
            pltpu.VMEM((CHUNKS, rows, 2 * FR, width), BF16),
            pltpu.VMEM((2, m // FINE, block_cols), F32),
            pltpu.VMEM((2, FINE, block_cols), F32),
            pltpu.VMEM((2, m, block_cols), BF16),
            pltpu.VMEM((2, rows * 2 * FR, block_cols), F32),
            pltpu.VMEM((rows, 8, 128), F32),
            dma((CHUNKS,)),
            dma((CHUNKS,)),
            dma((CHUNKS,)),
            dma((CHUNKS, chips - 1)),
            dma((CHUNKS, chips - 1)),
            dma((CHUNKS, 2, rows)),
            dma((CHUNKS, rows)),
            dma((rows - 1,)),
            dma((rows - 1,)),
        ],
        compiler_params=pltpu.CompilerParams(
            collective_id=0, has_side_effects=True, vmem_limit_bytes=60 * 1024 * 1024),
    )(visibilities, *small)


def solution(mesh):
    in_specs = (P(None, "col", "row"), P("col"), P(), P(), P(), P("col", "row"))
    out_specs = (P("col", None, None, "row"), P("col"))
    body = functools.partial(local, mesh.shape["col"], mesh.shape["row"])
    return jax.shard_map(body, mesh=mesh, in_specs=in_specs, out_specs=out_specs, check_vma=False)
```
